256 devices in a mesh: dp: 8 (over y, core), vocab: 32 (over x, z).
Axes of the slice: x: 4, y: 4, z: 8, core: 2. Of those that a mesh axis runs over, the one named last changes fastest.
Arguments:
- student_hidden: bfloat16 [4096, 2048], P('dp', 'vocab'), may hold values from -150 to 150
- teacher_hidden: bfloat16 [4096, 2048], P('dp', 'vocab'), may hold values from -150 to 150
- head: bfloat16 [2048, 65536], P(None, 'vocab'), may hold values from -0.375 to 0.375
- mask: int32 [4096], P('dp'), may hold values from 0 to 1
- steps: int32 [32], P('dp'), may hold values from 1 to 8
Outputs:
- divergence: float32 [4096], P('dp')
- hidden_grad: bfloat16 [4096, 2048], P('dp', 'vocab')
The draws below stay inside these ranges and needn't reach their ends.
All inputs are finite; a program needn't handle non-finite values.
Results may differ from the reference program's by a relative error of at most 0.0051.
Values may be sent and summed in bfloat16 or wider, within the bound.
No kernel may reach another device: no remote copies, remote signals or barrier semaphores. Data moves between devices by JAX's collectives and lax.ppermute only.
A program may use at most 64 MiB of HBM per device.

```python
import jax
import jax.numpy as jnp
from jax import lax

D = 2048
LENGTH = 128
STEPS = 8
TOK_DEV = 512
SEQS = 32
TOKENS = 4096
VOCAB = 65536


def hidden_pair(key):
    shared = jnp.clip(jax.random.normal(jax.random.fold_in(key, 11), (TOKENS, D), jnp.float32), -4.0, 4.0)
    student_own = jnp.clip(jax.random.normal(jax.random.fold_in(key, 13), (TOKENS, D), jnp.float32), -4.0, 4.0)
    teacher_own = jnp.clip(jax.random.normal(jax.random.fold_in(key, 17), (TOKENS, D), jnp.float32), -4.0, 4.0)
    student = 0.8 * shared + 0.6 * student_own
    teacher = 0.8 * shared + 0.6 * teacher_own
    return (student, teacher)


def draw_student_hidden(key, part):
    return hidden_pair(key)[0].astype(jnp.bfloat16)


def draw_teacher_hidden(key, part):
    return hidden_pair(key)[1].astype(jnp.bfloat16)


def noise_pair(key):
    sequence = jnp.arange(SEQS, dtype=jnp.int32)
    jitter = jax.random.randint(jax.random.fold_in(key, 31), (SEQS,), 0, 2).astype(jnp.int32)
    noise_steps = jnp.minimum(1 + STEPS * sequence // SEQS + jitter, STEPS).astype(jnp.int32)
    levels = jax.random.randint(jax.random.fold_in(key, 37), (TOKENS,), 0, STEPS).astype(jnp.int32)
    masked = (levels < jnp.repeat(noise_steps, LENGTH)).astype(jnp.int32)
    return (masked, noise_steps)


def draw_mask(key, part):
    return noise_pair(key)[0]


def draw_steps(key, part):
    return noise_pair(key)[1]


def block_scale(own_key, extent, cuts, smallest, high):
    gain, own = 1.0, jax.random.fold_in(own_key, 6)
    for position, blocks in cuts:
        steps = jnp.exp(jax.random.uniform(jax.random.fold_in(own, position), (blocks,), jnp.float32, smallest / len(cuts), high / len(cuts)))
        gain = gain * jnp.repeat(steps, extent[position] // blocks).reshape([-1 if axis == position else 1 for axis in range(len(extent))])
    return gain


def scatter_about(rng, dims, deviation, reach, shards=(), kind=jnp.bfloat16):
    values = deviation * jax.random.normal(rng, dims, jnp.float32)
    if shards:
        values = values * block_scale(rng, dims, shards, -0.22, 0.18)
    return jnp.clip(values, -reach, reach).astype(kind)


def setup_inputs(seed: int = 0) -> dict:
    key_of = jax.random.split(jax.random.key(seed), 6)
    return {
        "student_hidden": draw_student_hidden(jax.random.fold_in(key_of[5], 71), 0),
        "teacher_hidden": draw_teacher_hidden(jax.random.fold_in(key_of[5], 71), 0),
        "head": scatter_about(key_of[2], (D, VOCAB), (D // 9) ** -0.5, 0.375, ((1, 32),)),
        "mask": draw_mask(jax.random.fold_in(key_of[5], 71), 0),
        "steps": draw_steps(jax.random.fold_in(key_of[5], 71), 0),
    }


def token_weights(mask, steps):
    masked = mask.astype(jnp.float32)
    factor = jnp.repeat(STEPS / steps.astype(jnp.float32), LENGTH)
    count = jnp.sum(masked)
    return masked * factor * (TOKENS / jnp.maximum(count, 1.0))


def reference(student_hidden, teacher_hidden, head, mask, steps):
    weight = token_weights(mask, steps)
    blocks = TOKENS // TOK_DEV

    def one_block(inputs):
        student_rows, teacher_rows, weight_rows = inputs
        student_log = jnp.dot(student_rows, head, preferred_element_type=jnp.float32)
        teacher_log = jnp.dot(teacher_rows, head, preferred_element_type=jnp.float32)
        student_peak = jnp.max(student_log, axis=1, keepdims=True)
        teacher_peak = jnp.max(teacher_log, axis=1, keepdims=True)
        student_exp = jnp.exp(student_log - student_peak)
        teacher_exp = jnp.exp(teacher_log - teacher_peak)
        student_total = jnp.sum(student_exp, axis=1, keepdims=True)
        teacher_total = jnp.sum(teacher_exp, axis=1, keepdims=True)
        cross = jnp.sum(teacher_exp * (teacher_log - student_log), axis=1, keepdims=True)
        kl_rows = cross / teacher_total - (teacher_peak + jnp.log(teacher_total)) + (student_peak + jnp.log(student_total))
        slopes = (weight_rows[:, None] * (student_exp / student_total - teacher_exp / teacher_total)).astype(jnp.bfloat16)
        grad_rows = jnp.dot(slopes, head.T, preferred_element_type=jnp.float32).astype(jnp.bfloat16)
        return kl_rows[:, 0], grad_rows

    kl_blocks, grad_blocks = lax.map(one_block, (student_hidden.reshape(blocks, TOK_DEV, D), teacher_hidden.reshape(blocks, TOK_DEV, D), weight.reshape(blocks, TOK_DEV)))
    return kl_blocks.reshape(TOKENS), grad_blocks.reshape(TOKENS, D)
```

```python
import functools

import jax
import jax.numpy as jnp
from jax import lax
from jax.experimental import pallas as pl
from jax.experimental.pallas import tpu as pltpu
from jax.sharding import Mesh
from jax.sharding import PartitionSpec as P

LENGTH = 128
STEPS = 8
X, Z = 4, 8
TOK = 512
HALF = 256
FEAT = 64
D = 2048
VOC = 2048
TILE = 512
F32 = jnp.float32
BF16 = jnp.bfloat16


def shifted(value, axis, step):
    size = X if axis == "x" else Z
    return lax.ppermute(value, axis, [(i, (i + step) % size) for i in range(size)])


def sent_to_all(value, axis):
    copies = jnp.broadcast_to(value, (lax.axis_size(axis), *value.shape))
    return lax.all_to_all(copies, axis, split_axis=0, concat_axis=0, tiled=True)


def ring_of_eight(own, rows):
    ahead, behind = [own], [own]
    for _ in range(3):
        behind.append(shifted(behind[-1], "z", 1))
        ahead.append(shifted(ahead[-1], "z", -1))
    low = shifted(behind[-1][:rows], "z", 1)
    high = shifted(ahead[-1][rows:], "z", -1)
    return ahead, behind, low, high


def in_order(rotated, start):
    count = rotated.shape[0]
    return lax.dynamic_slice_in_dim(jnp.concatenate([rotated, rotated]), count - start, count)


def unpacked(blocks):
    count, rows, _ = blocks.shape
    parts = blocks.reshape(count, rows, 2, FEAT)
    return jnp.transpose(parts, (2, 1, 0, 3)).reshape(2 * rows, count * FEAT)


def gathered(student, teacher):
    x, z = lax.axis_index("x"), lax.axis_index("z")
    both = jnp.concatenate([student, teacher], axis=1)
    a, b = both[:HALF], both[HALF:]
    a_next, a_prev, a_far = shifted(a, "x", -1), shifted(a, "x", 1), shifted(a, "x", 2)
    b_ahead, b_behind, b_low, b_high = ring_of_eight(b, HALF // 2)
    own_a = unpacked(in_order(jnp.stack([a, a_next, a_far, a_prev]), x))
    a_ahead, a_behind, a_low, a_high = ring_of_eight(own_a, HALF)
    b_far = jnp.concatenate([b_low, b_high])
    own_b = unpacked(in_order(jnp.stack([*b_ahead, b_far, *b_behind[:0:-1]]), z))
    b_prev, b_next = shifted(own_b, "x", 1), shifted(own_b, "x", -1)
    far_low, far_high = shifted(b_prev[:HALF], "x", 1), shifted(b_next[HALF:], "x", -1)
    return (*a_ahead, a_low, a_high, *a_behind[:0:-1]), (own_b, b_next, far_low, far_high, b_prev)


def forward_kernel(place, *refs):
    a_refs, b_refs = refs[:9], refs[9:14]
    head_ref, student_ref, teacher_ref, stats_ref, state = refs[14:]
    step = pl.program_id(0)
    x, z = place[0], place[1]

    @pl.when(step == 0)
    def _():
        for row in (0, 2):
            state[row] = jnp.full((TOK, 128), -jnp.inf, F32)
        for row in (1, 3, 4):
            state[row] = jnp.zeros((TOK, 128), F32)

    a_rows = [r[...] for r in a_refs[:4]]
    a_rows.append(jnp.concatenate([a_refs[4][...], a_refs[5][...]], axis=0))
    a_rows += [r[...] for r in a_refs[6:]]
    weights = [head_ref[i, lax.rem(z + k, Z)] for k in range(Z) for i in range(X)]
    a_log = jnp.dot(
        jnp.concatenate(a_rows, axis=1),
        jnp.concatenate(weights, axis=0),
        preferred_element_type=F32,
    )
    b_far = jnp.concatenate([b_refs[2][...], b_refs[3][...]], axis=0)
    b_rows = [b_refs[0][...], b_refs[1][...], b_far, b_refs[4][...]]
    weights = [head_ref[lax.rem(x + k, X)].reshape(Z * FEAT, TILE) for k in range(X)]
    b_log = jnp.dot(
        jnp.concatenate(b_rows, axis=1),
        jnp.concatenate(weights, axis=0),
        preferred_element_type=F32,
    )
    student_ref[:HALF] = a_log[:HALF]
    teacher_ref[:HALF] = a_log[HALF:]
    student_ref[HALF:] = b_log[:HALF]
    teacher_ref[HALF:] = b_log[HALF:]
    cols = [slice(c, c + 128) for c in range(0, TILE, 128)]
    s = [student_ref[:, c] for c in cols]
    t = [teacher_ref[:, c] for c in cols]
    s_peak = functools.reduce(jnp.maximum, s, state[0])
    t_peak = functools.reduce(jnp.maximum, t, state[2])
    s_total = state[1] * jnp.exp(state[0] - s_peak)
    t_scale = jnp.exp(state[2] - t_peak)
    t_total, cross = state[3] * t_scale, state[4] * t_scale
    for s_part, t_part in zip(s, t):
        s_total += jnp.exp(s_part - s_peak)
        t_exp = jnp.exp(t_part - t_peak)
        t_total += t_exp
        cross += t_exp * (t_part - s_part)
    for row, value in enumerate((s_peak, s_total, t_peak, t_total, cross)):
        state[row] = value

    @pl.when(step == pl.num_programs(0) - 1)
    def _():
        s_top = jnp.max(s_peak, axis=1, keepdims=True)
        t_top = jnp.max(t_peak, axis=1, keepdims=True)
        s_by, t_by = jnp.exp(s_peak - s_top), jnp.exp(t_peak - t_top)
        columns = [
            s_top,
            jnp.sum(s_total * s_by, axis=1, keepdims=True),
            t_top,
            jnp.sum(t_total * t_by, axis=1, keepdims=True),
            jnp.sum(cross * t_by, axis=1, keepdims=True),
        ]
        lane = lax.broadcasted_iota(jnp.int32, (TOK, 128), 1)
        table = jnp.zeros((TOK, 128), F32)
        for k, column in enumerate(columns):
            table = jnp.where(lane == k, column, table)
        stats_ref[...] = table.T[:8]


def whole(shape):
    return pl.BlockSpec(shape, lambda *_: (0,) * len(shape))


def forward(place, a_parts, b_parts, head):
    parts = (*a_parts, *b_parts)
    return pl.pallas_call(
        forward_kernel,
        grid_spec=pltpu.PrefetchScalarGridSpec(
            num_scalar_prefetch=1,
            grid=(VOC // TILE,),
            in_specs=[whole(p.shape) for p in parts]
            + [pl.BlockSpec((X, Z, FEAT, TILE), lambda n, _: (0, 0, 0, n))],
            out_specs=[
                pl.BlockSpec((TOK, TILE), lambda n, _: (0, n)),
                pl.BlockSpec((TOK, TILE), lambda n, _: (0, n)),
                whole((8, TOK)),
            ],
            scratch_shapes=[pltpu.VMEM((5, TOK, 128), F32)],
        ),
        out_shape=[
            jax.ShapeDtypeStruct((TOK, VOC), F32),
            jax.ShapeDtypeStruct((TOK, VOC), F32),
            jax.ShapeDtypeStruct((8, TOK), F32),
        ],
        compiler_params=pltpu.CompilerParams(vmem_limit_bytes=48 << 20),
        cost_estimate=pl.CostEstimate(
            flops=4 * TOK * D * VOC, bytes_accessed=20 << 20, transcendentals=0
        ),
        name="forward",
    )(place, *parts, head.reshape(X, Z, FEAT, VOC))


def first_backward_kernel(place, factors, student_ref, teacher_ref, head_ref, slopes_ref, out_ref, total):
    step = pl.program_id(0)
    table = jnp.concatenate([factors[...], jnp.zeros((120, TOK), F32)], axis=0).T
    s_exp = jnp.exp(student_ref[...] - table[:, 0:1]) * table[:, 1:2]
    t_exp = jnp.exp(teacher_ref[...] - table[:, 2:3]) * table[:, 3:4]
    slopes = (s_exp - t_exp).astype(BF16)
    slopes_ref[...] = slopes
    part = lax.dot_general(
        head_ref[...], slopes, (((1,), (1,)), ((), ())), preferred_element_type=F32
    )

    @pl.when(step == 0)
    def _():
        total[...] = part

    @pl.when(step > 0)
    def _():
        total[...] += part

    @pl.when(step == pl.num_programs(0) - 1)
    def _():
        out_ref[...] = total[...].astype(BF16)


def first_backward(place, factors, student_log, teacher_log, head):
    rows = D // X
    return pl.pallas_call(
        first_backward_kernel,
        grid_spec=pltpu.PrefetchScalarGridSpec(
            num_scalar_prefetch=1,
            grid=(VOC // TILE,),
            in_specs=[
                whole((8, TOK)),
                pl.BlockSpec((TOK, TILE), lambda n, _: (0, n)),
                pl.BlockSpec((TOK, TILE), lambda n, _: (0, n)),
                pl.BlockSpec((rows, TILE), lambda n, place: (lax.rem(place[0] + 2, X), n)),
            ],
            out_specs=[
                pl.BlockSpec((TOK, TILE), lambda n, _: (0, n)),
                whole((rows, TOK)),
            ],
            scratch_shapes=[pltpu.VMEM((rows, TOK), F32)],
        ),
        out_shape=[
            jax.ShapeDtypeStruct((TOK, VOC), BF16),
            jax.ShapeDtypeStruct((rows, TOK), BF16),
        ],
        compiler_params=pltpu.CompilerParams(vmem_limit_bytes=32 << 20),
        cost_estimate=pl.CostEstimate(
            flops=2 * TOK * rows * VOC, bytes_accessed=12 << 20, transcendentals=0
        ),
        name="first_backward",
    )(place, factors, student_log, teacher_log, head)


def rest_backward_kernel(place, slopes_ref, head_ref, out_ref):
    out_ref[0] = lax.dot_general(
        head_ref[...],
        slopes_ref[...],
        (((1,), (1,)), ((), ())),
        preferred_element_type=F32,
    ).astype(BF16)


def rest_backward(place, slopes, head):
    rows, cut = D // X, 2
    tall = rows // cut

    def head_at(n, place):
        turn = lax.rem(2 * lax.div(n, cut) + 1, 5)
        return (lax.rem(place[0] + turn, X) * cut + lax.rem(n, cut), 0)

    return pl.pallas_call(
        rest_backward_kernel,
        grid_spec=pltpu.PrefetchScalarGridSpec(
            num_scalar_prefetch=1,
            grid=(3 * cut,),
            in_specs=[whole((TOK, VOC)), pl.BlockSpec((tall, VOC), head_at)],
            out_specs=pl.BlockSpec((1, tall, TOK), lambda n, _: (lax.div(n, cut), lax.rem(n, cut), 0)),
        ),
        out_shape=jax.ShapeDtypeStruct((3, rows, TOK), BF16),
        compiler_params=pltpu.CompilerParams(vmem_limit_bytes=32 << 20),
        cost_estimate=pl.CostEstimate(
            flops=6 * TOK * rows * VOC, bytes_accessed=10 << 20, transcendentals=0
        ),
        name="rest_backward",
    )(place, slopes, head)


def merged(stats):
    s_peak, t_peak = jnp.max(stats[:, 0], axis=0), jnp.max(stats[:, 2], axis=0)
    s_by, t_by = jnp.exp(stats[:, 0] - s_peak), jnp.exp(stats[:, 2] - t_peak)
    return (
        s_peak,
        jnp.sum(stats[:, 1] * s_by, axis=0),
        t_peak,
        jnp.sum(stats[:, 3] * t_by, axis=0),
        jnp.sum(stats[:, 4] * t_by, axis=0),
    )


def reduced(far, prev_next_own):
    half = far.shape[0] // 2
    from_prev, from_next = shifted(far[:half], "x", 1), shifted(far[half:], "x", -1)
    to_next, to_prev, own = prev_next_own
    wide = lambda v: v.astype(F32)
    up = jnp.concatenate([(wide(to_next[:half]) + wide(from_prev)).astype(BF16), to_next[half:]])
    down = jnp.concatenate([to_prev[:half], (wide(to_prev[half:]) + wide(from_next)).astype(BF16)])
    total = wide(own) + wide(shifted(up, "x", 1)) + wide(shifted(down, "x", -1))
    pieces = total.astype(BF16).reshape(Z, FEAT, TOK)
    pieces = lax.all_to_all(pieces, "z", split_axis=0, concat_axis=0, tiled=True)
    return jnp.sum(wide(pieces), axis=0)


def per_device(student_hidden, teacher_hidden, head, mask, steps):
    rows = mask.shape[0]
    masked = mask.astype(F32)
    place = jnp.stack([lax.axis_index("x"), lax.axis_index("z")]).astype(jnp.int32)
    count = jnp.sum(sent_to_all(jnp.sum(masked), "dp"))
    factor = jnp.repeat(STEPS / steps.astype(F32), LENGTH)
    weight = masked * factor * (rows * lax.axis_size("dp") / jnp.maximum(count, 1.0))
    a_parts, b_parts = gathered(student_hidden, teacher_hidden)
    student_log, teacher_log, stats = forward(place, a_parts, b_parts, head)
    stats = jnp.stack(merged(sent_to_all(stats[:5], "x")))
    student_peak, student_total, teacher_peak, teacher_total, cross = merged(sent_to_all(stats, "z"))
    divergence = (
        cross / teacher_total
        - (teacher_peak + jnp.log(teacher_total))
        + (student_peak + jnp.log(student_total))
    )
    zero = jnp.zeros_like(weight)
    factors = jnp.stack(
        [student_peak, weight / student_total, teacher_peak, weight / teacher_total, zero, zero, zero, zero]
    )
    slopes, far = first_backward(place, factors, student_log, teacher_log, head)
    rest = rest_backward(place, slopes, head)
    summed = reduced(far, rest)
    return (divergence, summed.T.astype(BF16))


def solution(mesh):
    torus = Mesh(mesh.devices.reshape(mesh.shape["dp"], X, Z), ("dp", "x", "z"))
    split = ("x", "z")
    in_specs = (P("dp", split), P("dp", split), P(None, split), P("dp"), P("dp"))
    out_specs = (P("dp"), P("dp", split))
    return jax.shard_map(
        per_device, mesh=torus, in_specs=in_specs, out_specs=out_specs, check_vma=False
    )
```

```python
import functools

import jax
import jax.numpy as jnp
from jax import lax
from jax.experimental import pallas as pl
from jax.experimental.pallas import tpu as pltpu
from jax.sharding import Mesh
from jax.sharding import PartitionSpec as P

LENGTH = 128
STEPS = 8
X, Z = 4, 8
TOK = 512
HALF = 256
FEAT = 64
D = 2048
VOC = 2048
TILE = 512
F32 = jnp.float32
BF16 = jnp.bfloat16


def shifted(value, axis, step):
    size = X if axis == "x" else Z
    return lax.ppermute(value, axis, [(i, (i + step) % size) for i in range(size)])


def exchanged(value, axis):
    return lax.all_to_all(value, axis, split_axis=0, concat_axis=0, tiled=True)


def local(kernel, shapes, limit, name, *values):
    return pl.pallas_call(
        kernel,
        out_shape=[jax.ShapeDtypeStruct(shape, kind) for shape, kind in shapes],
        compiler_params=pltpu.CompilerParams(vmem_limit_bytes=limit << 20),
        name=name,
    )(*values)


def entry_kernel(student_ref, teacher_ref, mask_ref, a_ref, b_ref, count_ref):
    both = jnp.concatenate([student_ref[...], teacher_ref[...]], axis=0).T
    a_ref[...] = both[:HALF]
    b_ref[...] = jnp.broadcast_to(both[HALF:], b_ref.shape)
    count_ref[...] = jnp.full((8, 128), jnp.sum(mask_ref[...].astype(F32)))


def side_by_side(blocks, out_ref):
    for lanes, rows in ((slice(0, FEAT), slice(0, HALF)), (slice(FEAT, None), slice(HALF, None))):
        out_ref[rows] = jnp.concatenate([block[:, lanes] for block in blocks], axis=1)


def pack_a_kernel(*refs):
    side_by_side([ref[...] for ref in refs[:-1]], refs[-1])


def pack_b_kernel(blocks_ref, out_ref):
    side_by_side([blocks_ref[k] for k in range(Z)], out_ref)


def tied(*values):
    return lax.optimization_barrier(values)


def added_over_dp(count, bit):
    pairs = [(i, i ^ bit) for i in range(lax.axis_size("dp"))]
    return count + lax.ppermute(count, "dp", pairs)


def gathered(a, b, count):
    a_next, a_prev, a_far = shifted(a, "x", -1), shifted(a, "x", 1), shifted(a, "x", 2)
    b = exchanged(b, "z")
    packed = [((2 * HALF, X * FEAT), BF16)]
    (own_a,) = local(pack_a_kernel, packed, 4, "pack_a", a, a_next, a_far, a_prev)
    own_a, count = tied(own_a, added_over_dp(count, 1))
    ahead, behind = [own_a], [own_a]
    for hop in range(3):
        if hop:
            behind[-1], ahead[-1], count = tied(behind[-1], ahead[-1], added_over_dp(count, 2 * hop))
        behind.append(shifted(behind[-1], "z", 1))
        ahead.append(shifted(ahead[-1], "z", -1))
    low, high = shifted(behind[-1][:HALF], "z", 1), shifted(ahead[-1][HALF:], "z", -1)
    packed = [((2 * HALF, Z * FEAT), BF16)]
    (own_b,) = local(pack_b_kernel, packed, 4, "pack_b", b)
    b_prev, b_next = shifted(own_b, "x", 1), shifted(own_b, "x", -1)
    far_low, far_high = shifted(b_prev[:HALF], "x", 1), shifted(b_next[HALF:], "x", -1)
    return (*ahead, low, high, *behind[:0:-1]), (own_b, b_next, far_low, far_high, b_prev), count


def forward_kernel(place, *refs):
    a_refs, b_refs = refs[:9], refs[9:14]
    count_ref, mask_ref, head_ref, student_ref, teacher_ref, stats_ref, state = refs[14:]
    step = pl.program_id(0)
    x, z = place[0], place[1]

    @pl.when(step == 0)
    def _():
        for row in (0, 2):
            state[row] = jnp.full((TOK, 128), -jnp.inf, F32)
        for row in (1, 3, 4):
            state[row] = jnp.zeros((TOK, 128), F32)

    a_rows = [r[...] for r in a_refs[:4]]
    a_rows.append(jnp.concatenate([a_refs[4][...], a_refs[5][...]], axis=0))
    a_rows += [r[...] for r in a_refs[6:]]
    weights = [head_ref[lax.rem(x + i, X), lax.rem(z + k, Z)] for k in range(Z) for i in range(X)]
    a_log = jnp.dot(
        jnp.concatenate(a_rows, axis=1),
        jnp.concatenate(weights, axis=0),
        preferred_element_type=F32,
    )
    b_far = jnp.concatenate([b_refs[2][...], b_refs[3][...]], axis=0)
    b_rows = [b_refs[0][...], b_refs[1][...], b_far, b_refs[4][...]]
    weights = [head_ref[lax.rem(x + k, X), i] for k in range(X) for i in range(Z)]
    b_log = jnp.dot(
        jnp.concatenate(b_rows, axis=1),
        jnp.concatenate(weights, axis=0),
        preferred_element_type=F32,
    )
    student_ref[:HALF] = a_log[:HALF]
    teacher_ref[:HALF] = a_log[HALF:]
    student_ref[HALF:] = b_log[:HALF]
    teacher_ref[HALF:] = b_log[HALF:]
    cols = [slice(c, c + 128) for c in range(0, TILE, 128)]
    s = [student_ref[:, c] for c in cols]
    t = [teacher_ref[:, c] for c in cols]
    s_peak = functools.reduce(jnp.maximum, s, state[0])
    t_peak = functools.reduce(jnp.maximum, t, state[2])
    s_total = state[1] * jnp.exp(state[0] - s_peak)
    t_scale = jnp.exp(state[2] - t_peak)
    t_total, cross = state[3] * t_scale, state[4] * t_scale
    for s_part, t_part in zip(s, t):
        s_total += jnp.exp(s_part - s_peak)
        t_exp = jnp.exp(t_part - t_peak)
        t_total += t_exp
        cross += t_exp * (t_part - s_part)
    for row, value in enumerate((s_peak, s_total, t_peak, t_total, cross)):
        state[row] = value

    @pl.when(step == pl.num_programs(0) - 1)
    def _():
        s_top = jnp.max(s_peak, axis=1, keepdims=True)
        t_top = jnp.max(t_peak, axis=1, keepdims=True)
        s_by, t_by = jnp.exp(s_peak - s_top), jnp.exp(t_peak - t_top)
        columns = [
            s_top,
            jnp.sum(s_total * s_by, axis=1, keepdims=True),
            t_top,
            jnp.sum(t_total * t_by, axis=1, keepdims=True),
            jnp.sum(cross * t_by, axis=1, keepdims=True),
        ]
        lane = lax.broadcasted_iota(jnp.int32, (TOK, 128), 1)
        table = jnp.zeros((TOK, 128), F32)
        for k, column in enumerate(columns):
            table = jnp.where(lane == k, column, table)
        token = lax.broadcasted_iota(jnp.int32, (1, TOK), 1)
        steps = jnp.full((1, TOK), place[2])
        for k in range(1, TOK // LENGTH):
            steps = jnp.where(token >= k * LENGTH, place[2 + k], steps)
        factor = STEPS / steps.astype(F32)
        scale = float(8 * TOK) / jnp.maximum(count_ref[0:1, 0:1], 1.0)
        weight = mask_ref[...].astype(F32) * factor * scale
        rows = jnp.concatenate([table.T[:5], weight, jnp.zeros((2, TOK), F32)], axis=0)
        stats_ref[...] = jnp.broadcast_to(rows, (X, 8, TOK))


def whole(shape):
    return pl.BlockSpec(shape, lambda *_: (0,) * len(shape))


def forward(place, a_parts, b_parts, count, mask, head):
    parts = (*a_parts, *b_parts, count, mask)
    return pl.pallas_call(
        forward_kernel,
        grid_spec=pltpu.PrefetchScalarGridSpec(
            num_scalar_prefetch=1,
            grid=(VOC // TILE,),
            in_specs=[whole(p.shape) for p in parts]
            + [pl.BlockSpec((X, Z, FEAT, TILE), lambda n, _: (0, 0, 0, n))],
            out_specs=[
                pl.BlockSpec((TOK, TILE), lambda n, _: (0, n)),
                pl.BlockSpec((TOK, TILE), lambda n, _: (0, n)),
                whole((X, 8, TOK)),
            ],
            scratch_shapes=[pltpu.VMEM((5, TOK, 128), F32)],
        ),
        out_shape=[
            jax.ShapeDtypeStruct((TOK, VOC), F32),
            jax.ShapeDtypeStruct((TOK, VOC), F32),
            jax.ShapeDtypeStruct((X, 8, TOK), F32),
        ],
        compiler_params=pltpu.CompilerParams(vmem_limit_bytes=18 << 20),
        cost_estimate=pl.CostEstimate(
            flops=4 * TOK * D * VOC, bytes_accessed=4 << 20, transcendentals=0
        ),
        name="forward",
    )(place, *parts, head.reshape(X, Z, FEAT, VOC))


def merged(stats_ref, count):
    rows = [[stats_ref[k, row : row + 1] for k in range(count)] for row in range(5)]
    s_peak = functools.reduce(jnp.maximum, rows[0])
    t_peak = functools.reduce(jnp.maximum, rows[2])
    s_by = [jnp.exp(peak - s_peak) for peak in rows[0]]
    t_by = [jnp.exp(peak - t_peak) for peak in rows[2]]
    s_total = sum(total * by for total, by in zip(rows[1], s_by))
    t_total = sum(total * by for total, by in zip(rows[3], t_by))
    cross = sum(total * by for total, by in zip(rows[4], t_by))
    return s_peak, s_total, t_peak, t_total, cross


def merge_kernel(stats_ref, out_ref):
    rest = [stats_ref[0, 5:6], jnp.zeros((2, TOK), F32)]
    joined = jnp.concatenate([*merged(stats_ref, X), *rest], axis=0)
    out_ref[...] = jnp.broadcast_to(joined, (Z, 8, TOK))


def first_backward_kernel(
    place, stats_ref, student_ref, teacher_ref, head_ref,
    slopes_ref, out_ref, kl_ref, total, table_ref,
):
    step = pl.program_id(0)

    @pl.when(step == 0)
    def _():
        s_peak, s_total, t_peak, t_total, cross = merged(stats_ref, Z)
        kl_ref[...] = cross / t_total - (t_peak + jnp.log(t_total)) + (s_peak + jnp.log(s_total))
        weight = stats_ref[0, 5:6]
        rows = [s_peak, weight / s_total, t_peak, weight / t_total, jnp.zeros((124, TOK), F32)]
        table_ref[...] = jnp.concatenate(rows, axis=0).T

    s_exp = jnp.exp(student_ref[...] - table_ref[:, 0:1]) * table_ref[:, 1:2]
    t_exp = jnp.exp(teacher_ref[...] - table_ref[:, 2:3]) * table_ref[:, 3:4]
    slopes = (s_exp - t_exp).astype(BF16)
    slopes_ref[...] = slopes
    part = lax.dot_general(
        head_ref[...], slopes, (((1,), (1,)), ((), ())), preferred_element_type=F32
    )

    @pl.when(step == 0)
    def _():
        total[...] = part

    @pl.when(step > 0)
    def _():
        total[...] += part

    @pl.when(step == pl.num_programs(0) - 1)
    def _():
        out_ref[...] = total[...].astype(BF16)


def first_backward(place, stats, student_log, teacher_log, head):
    rows = D // X
    return pl.pallas_call(
        first_backward_kernel,
        grid_spec=pltpu.PrefetchScalarGridSpec(
            num_scalar_prefetch=1,
            grid=(VOC // TILE,),
            in_specs=[
                whole((Z, 8, TOK)),
                pl.BlockSpec((TOK, TILE), lambda n, _: (0, n)),
                pl.BlockSpec((TOK, TILE), lambda n, _: (0, n)),
                pl.BlockSpec((rows, TILE), lambda n, place: (lax.rem(place[0] + 2, X), n)),
            ],
            out_specs=[
                pl.BlockSpec((TOK, TILE), lambda n, _: (0, n)),
                whole((rows, TOK)),
                whole((1, TOK)),
            ],
            scratch_shapes=[pltpu.VMEM((rows, TOK), F32), pltpu.VMEM((TOK, 128), F32)],
        ),
        out_shape=[
            jax.ShapeDtypeStruct((TOK, VOC), BF16),
            jax.ShapeDtypeStruct((rows, TOK), BF16),
            jax.ShapeDtypeStruct((1, TOK), F32),
        ],
        compiler_params=pltpu.CompilerParams(vmem_limit_bytes=12 << 20),
        cost_estimate=pl.CostEstimate(
            flops=2 * TOK * rows * VOC, bytes_accessed=12 << 20, transcendentals=0
        ),
        name="first_backward",
    )(place, stats, student_log, teacher_log, head)


def rest_backward_kernel(place, slopes_ref, head_ref, out_ref):
    out_ref[0] = lax.dot_general(
        head_ref[...],
        slopes_ref[...],
        (((1,), (1,)), ((), ())),
        preferred_element_type=F32,
    ).astype(BF16)


def rest_backward(place, slopes, head):
    rows, cut = D // X, 2
    tall = rows // cut

    def head_at(n, place):
        turn = lax.rem(2 * lax.div(n, cut) + 1, 5)
        return (lax.rem(place[0] + turn, X) * cut + lax.rem(n, cut), 0)

    return pl.pallas_call(
        rest_backward_kernel,
        grid_spec=pltpu.PrefetchScalarGridSpec(
            num_scalar_prefetch=1,
            grid=(3 * cut,),
            in_specs=[whole((TOK, VOC)), pl.BlockSpec((tall, VOC), head_at)],
            out_specs=pl.BlockSpec((1, tall, TOK), lambda n, _: (lax.div(n, cut), lax.rem(n, cut), 0)),
        ),
        out_shape=jax.ShapeDtypeStruct((3, rows, TOK), BF16),
        compiler_params=pltpu.CompilerParams(vmem_limit_bytes=4 << 20),
        cost_estimate=pl.CostEstimate(
            flops=6 * TOK * rows * VOC, bytes_accessed=10 << 20, transcendentals=0
        ),
        name="rest_backward",
    )(place, slopes, head)


def reduced(far, prev_next_own):
    half = far.shape[0] // 2
    from_prev, from_next = shifted(far[:half], "x", 1), shifted(far[half:], "x", -1)
    to_next, to_prev, own = prev_next_own
    wide = lambda v: v.astype(F32)
    up = jnp.concatenate([(wide(to_next[:half]) + wide(from_prev)).astype(BF16), to_next[half:]])
    down = jnp.concatenate([to_prev[:half], (wide(to_prev[half:]) + wide(from_next)).astype(BF16)])
    total = wide(own) + wide(shifted(up, "x", 1)) + wide(shifted(down, "x", -1))
    pieces = total.astype(BF16).reshape(Z, FEAT, TOK)
    pieces = lax.all_to_all(pieces, "z", split_axis=0, concat_axis=0, tiled=True)
    return jnp.sum(wide(pieces), axis=0)


def per_device(student_hidden, teacher_hidden, head, mask, steps):
    row = mask.reshape(1, TOK)
    half, block = (HALF, 2 * FEAT), (8, 128)
    here = jnp.stack([lax.axis_index("x"), lax.axis_index("z")]).astype(jnp.int32)
    place, row = tied(jnp.concatenate([here, steps]), row)
    a, b, count = local(
        entry_kernel, [(half, BF16), ((Z, *half), BF16), (block, F32)], 4, "entry",
        student_hidden.T, teacher_hidden.T, row,
    )
    a_parts, b_parts, count = gathered(a, b, count)
    student_log, teacher_log, stats = forward(place, a_parts, b_parts, count, row, head)
    stats = exchanged(stats, "x")
    (stats,) = local(merge_kernel, [((Z, 8, TOK), F32)], 4, "merge_x", stats)
    stats = exchanged(stats, "z")
    slopes, far, divergence = first_backward(place, stats, student_log, teacher_log, head)
    rest = rest_backward(place, slopes, head)
    summed = reduced(far, rest)
    return (divergence[0], summed.T.astype(BF16))


def solution(mesh):
    torus = Mesh(mesh.devices.reshape(mesh.shape["dp"], X, Z), ("dp", "x", "z"))
    split = ("x", "z")
    in_specs = (P("dp", split), P("dp", split), P(None, split), P("dp"), P("dp"))
    out_specs = (P("dp"), P("dp", split))
    return jax.shard_map(
        per_device, mesh=torus, in_specs=in_specs, out_specs=out_specs, check_vma=False
    )
```

```python
import functools

import jax
import jax.numpy as jnp
from jax import lax
from jax.experimental import pallas as pl
from jax.experimental.pallas import tpu as pltpu
from jax.sharding import Mesh
from jax.sharding import PartitionSpec as P

LENGTH = 128
STEPS = 8
X, Z = 4, 8
TOK = 512
HALF = 256
FEAT = 64
D = 2048
VOC = 2048
TILE = 512
FORWARD_LIMIT = 22
BACKWARD_LIMIT = 24
RESIDENT_LIMIT = 44
F32 = jnp.float32
BF16 = jnp.bfloat16


def shifted(value, axis, step):
    size = X if axis == "x" else Z
    return lax.ppermute(value, axis, [(i, (i + step) % size) for i in range(size)])


def exchanged(value, axis):
    return lax.all_to_all(value, axis, split_axis=0, concat_axis=0, tiled=True)


def local(kernel, shapes, limit, name, *values):
    return pl.pallas_call(
        kernel,
        out_shape=[jax.ShapeDtypeStruct(shape, kind) for shape, kind in shapes],
        compiler_params=pltpu.CompilerParams(vmem_limit_bytes=limit << 20),
        name=name,
    )(*values)


def entry_kernel(student_ref, teacher_ref, mask_ref, a_ref, b_ref, count_ref):
    both = jnp.concatenate([student_ref[...], teacher_ref[...]], axis=0).T
    a_ref[...] = both[:HALF]
    b_ref[...] = jnp.broadcast_to(both[HALF:], b_ref.shape)
    count_ref[...] = jnp.full((8, 128), jnp.sum(mask_ref[...].astype(F32)))


def side_by_side(blocks, out_ref):
    for lanes, rows in ((slice(0, FEAT), slice(0, HALF)), (slice(FEAT, None), slice(HALF, None))):
        out_ref[rows] = jnp.concatenate([block[:, lanes] for block in blocks], axis=1)


def pack_a_kernel(*refs):
    side_by_side([ref[...] for ref in refs[:-1]], refs[-1])


def pack_b_kernel(place_ref, blocks_ref, out_ref):
    side_by_side([blocks_ref[lax.rem(place_ref[1] + k, Z)] for k in range(Z)], out_ref)


def pack_b(place, blocks):
    return pl.pallas_call(
        pack_b_kernel,
        in_specs=[pl.BlockSpec(memory_space=pltpu.SMEM), pl.BlockSpec(memory_space=pltpu.VMEM)],
        out_shape=jax.ShapeDtypeStruct((2 * HALF, Z * FEAT), BF16),
        compiler_params=pltpu.CompilerParams(vmem_limit_bytes=4 << 20),
        name="pack_b",
    )(place, blocks)


def tied(*values):
    return lax.optimization_barrier(values)


def added_over_dp(count, bit):
    pairs = [(i, i ^ bit) for i in range(lax.axis_size("dp"))]
    return count + lax.ppermute(count, "dp", pairs)


def gathered(place, a, b, count, head):
    a_next, a_prev, a_far = shifted(a, "x", -1), shifted(a, "x", 1), shifted(a, "x", 2)
    b = exchanged(b, "z")
    a_next, place = tied(a_next, place)
    packed = [((2 * HALF, X * FEAT), BF16)]
    (own_a,) = local(pack_a_kernel, packed, 4, "pack_a", a, a_next, a_far, a_prev)
    own_b, head, count = tied(pack_b(place, b), head, added_over_dp(count, 1))
    head = resident(head)
    ahead, behind = [own_a], [own_a]
    for hop in range(3):
        if hop == 2:
            count = added_over_dp(count, 2)
            behind[-1], ahead[-1], count, head = tied(behind[-1], ahead[-1], count, head)
        behind.append(shifted(behind[-1], "z", 1))
        ahead.append(shifted(ahead[-1], "z", -1))
    behind[-1], ahead[-1], count = tied(behind[-1], ahead[-1], added_over_dp(count, 4))
    low, high = shifted(behind[-1][:HALF], "z", 1), shifted(ahead[-1][HALF:], "z", -1)
    b_prev, b_next = shifted(own_b, "x", 1), shifted(own_b, "x", -1)
    far_low, far_high = shifted(b_prev[:HALF], "x", 1), shifted(b_next[HALF:], "x", -1)
    return (*ahead, low, high, *behind[:0:-1], own_b, b_next, far_low, far_high, b_prev), place, count, head


def resident_kernel(head_ref, out_ref, done):
    copy = pltpu.make_async_copy(head_ref, out_ref, done)
    copy.start()
    copy.wait()


def resident(head):
    return pl.pallas_call(
        resident_kernel,
        in_specs=[pl.BlockSpec(memory_space=pl.ANY)],
        out_specs=pl.BlockSpec(memory_space=pltpu.VMEM),
        out_shape=jax.ShapeDtypeStruct(head.shape, head.dtype),
        scratch_shapes=[pltpu.SemaphoreType.DMA],
        compiler_params=pltpu.CompilerParams(vmem_limit_bytes=RESIDENT_LIMIT << 20),
        cost_estimate=pl.CostEstimate(flops=3 << 30, bytes_accessed=16 << 20, transcendentals=0),
        name="resident",
    )(head)


def whole(shape):
    return pl.BlockSpec(shape, lambda *_: (0,) * len(shape))


def interleaved(pieces, rows_ref):
    lane = lax.broadcasted_iota(jnp.int32, (2 * HALF, 128), 1)
    for pair in range(Z // 2):
        tiles = [piece[:, pair * 128 : pair * 128 + 128] for piece in pieces]
        turned = [jnp.concatenate([t[:, FEAT:], t[:, :FEAT]], axis=1) for t in tiles]
        for side, (lower, upper) in enumerate(((tiles, turned), (turned, tiles))):
            at = (2 * pair + side) * X * FEAT
            for i in range(0, X, 2):
                both = jnp.where(lane < FEAT, lower[i], upper[i + 1])
                rows_ref[2 * HALF :, at + i * FEAT : at + i * FEAT + 128] = both


def tile_stats(student_ref, teacher_ref, n, state):
    cols = [slice(c, c + 128) for c in range(n * TILE, (n + 1) * TILE, 128)]
    s_old, s_total, t_old, t_total, cross = state
    s_peak = functools.reduce(jnp.maximum, [student_ref[:, c] for c in cols], s_old)
    t_peak = functools.reduce(jnp.maximum, [teacher_ref[:, c] for c in cols], t_old)
    s_total = s_total * jnp.exp(s_old - s_peak)
    t_scale = jnp.exp(t_old - t_peak)
    t_total, cross = t_total * t_scale, cross * t_scale
    for c in cols:
        s_part, t_part = student_ref[:, c], teacher_ref[:, c]
        s_exp, t_exp = jnp.exp(s_part - s_peak), jnp.exp(t_part - t_peak)
        s_total += s_exp
        t_total += t_exp
        cross += t_exp * (t_part - s_part)
        student_ref[:, c] = s_exp
        teacher_ref[:, c] = t_exp
    return s_peak, s_total, t_peak, t_total, cross


def forward_kernel(place, *refs):
    a_refs, b_refs = refs[:9], refs[9:14]
    count_ref, mask_ref, head_ref, student_ref, teacher_ref = refs[14:19]
    stats_ref, s_tile_ref, t_tile_ref, state_ref, rows_ref = refs[19:]
    x, z = place[0], place[1]
    width = X * FEAT
    for k, ref in enumerate((*a_refs[:4], None, *a_refs[6:])):
        if ref is not None:
            rows_ref[: 2 * HALF, k * width : (k + 1) * width] = ref[...]
    rows_ref[:HALF, 4 * width : 5 * width] = a_refs[4][...]
    rows_ref[HALF : 2 * HALF, 4 * width : 5 * width] = a_refs[5][...]
    b_far = jnp.concatenate([b_refs[2][...], b_refs[3][...]], axis=0)
    interleaved([b_refs[0][...], b_refs[1][...], b_far, b_refs[4][...]], rows_ref)

    def multiply(n):
        cols = slice(n * TILE, (n + 1) * TILE)
        weights = [
            head_ref[lax.rem(x + i, X), lax.rem(z + k, Z), :, cols]
            for k in range(Z)
            for i in range(X)
        ]
        logs = jnp.dot(rows_ref[...], jnp.concatenate(weights, axis=0), preferred_element_type=F32)
        student_ref[:HALF, cols] = logs[:HALF]
        teacher_ref[:HALF, cols] = logs[HALF : 2 * HALF]
        student_ref[HALF:, cols] = logs[2 * HALF : 3 * HALF]
        teacher_ref[HALF:, cols] = logs[3 * HALF :]

    def summarize(n):
        if n:
            state = [state_ref[row] for row in range(5)]
        else:
            low, zero = jnp.full((TOK, 128), -jnp.inf, F32), jnp.zeros((TOK, 128), F32)
            state = [low, zero, low, zero, zero]
        state = tile_stats(student_ref, teacher_ref, n, state)
        for row, value in enumerate(state):
            state_ref[row] = value
        s_tile_ref[n], t_tile_ref[n] = state[0], state[2]

    tiles = VOC // TILE
    for n in range(tiles + 1):
        if n < tiles:
            multiply(n)
        if n:
            summarize(n - 1)

    s_peak, s_total, t_peak, t_total, cross = [state_ref[row] for row in range(5)]
    s_top = jnp.max(s_peak, axis=1, keepdims=True)
    t_top = jnp.max(t_peak, axis=1, keepdims=True)
    s_by, t_by = jnp.exp(s_peak - s_top), jnp.exp(t_peak - t_top)
    columns = [
        s_top,
        jnp.sum(s_total * s_by, axis=1, keepdims=True),
        t_top,
        jnp.sum(t_total * t_by, axis=1, keepdims=True),
        jnp.sum(cross * t_by, axis=1, keepdims=True),
    ]
    lane = lax.broadcasted_iota(jnp.int32, (TOK, 128), 1)
    table = jnp.zeros((TOK, 128), F32)
    for k, column in enumerate(columns):
        table = jnp.where(lane == k, column, table)
    token = lax.broadcasted_iota(jnp.int32, (1, TOK), 1)
    steps = jnp.full((1, TOK), place[2])
    for k in range(1, TOK // LENGTH):
        steps = jnp.where(token >= k * LENGTH, place[2 + k], steps)
    factor = STEPS / steps.astype(F32)
    scale = float(8 * TOK) / jnp.maximum(count_ref[0:1, 0:1], 1.0)
    weight = mask_ref[...].astype(F32) * factor * scale
    rows = jnp.concatenate([table.T[:5], weight, jnp.zeros((2, TOK), F32)], axis=0)
    stats_ref[...] = jnp.broadcast_to(rows, (X, 8, TOK))


def forward(place, parts, count, mask, head):
    values = (*parts, count, mask)
    tiles = VOC // TILE
    logs = jax.ShapeDtypeStruct((TOK, VOC), F32)
    peaks = jax.ShapeDtypeStruct((tiles, TOK, 128), F32)
    return pl.pallas_call(
        forward_kernel,
        grid_spec=pltpu.PrefetchScalarGridSpec(
            num_scalar_prefetch=1,
            grid=(1,),
            in_specs=[whole(v.shape) for v in values]
            + [whole((X, Z, FEAT, VOC))],
            out_specs=[
                whole((TOK, VOC)),
                whole((TOK, VOC)),
                whole((X, 8, TOK)),
                whole((tiles, TOK, 128)),
                whole((tiles, TOK, 128)),
            ],
            scratch_shapes=[pltpu.VMEM((5, TOK, 128), F32), pltpu.VMEM((4 * HALF, D), BF16)],
        ),
        out_shape=[logs, logs, jax.ShapeDtypeStruct((X, 8, TOK), F32), peaks, peaks],
        compiler_params=pltpu.CompilerParams(vmem_limit_bytes=FORWARD_LIMIT << 20),
        cost_estimate=pl.CostEstimate(
            flops=4 * TOK * D * VOC, bytes_accessed=4 << 20, transcendentals=0
        ),
        name="forward",
    )(place, *values, head.reshape(X, Z, FEAT, VOC))


def merged(stats_ref, count):
    rows = [[stats_ref[k, row : row + 1] for k in range(count)] for row in range(5)]
    s_peak = functools.reduce(jnp.maximum, rows[0])
    t_peak = functools.reduce(jnp.maximum, rows[2])
    s_by = [jnp.exp(peak - s_peak) for peak in rows[0]]
    t_by = [jnp.exp(peak - t_peak) for peak in rows[2]]
    s_total = sum(total * by for total, by in zip(rows[1], s_by))
    t_total = sum(total * by for total, by in zip(rows[3], t_by))
    cross = sum(total * by for total, by in zip(rows[4], t_by))
    return s_peak, s_total, t_peak, t_total, cross


def merge_kernel(stats_ref, out_ref):
    rest = [stats_ref[0, 5:6], jnp.zeros((2, TOK), F32)]
    joined = jnp.concatenate([*merged(stats_ref, X), *rest], axis=0)
    out_ref[...] = jnp.broadcast_to(joined, (Z, 8, TOK))


def first_backward_kernel(
    place, stats_ref, student_ref, teacher_ref, s_tile_ref, t_tile_ref, head_ref,
    slopes_ref, out_ref, kl_ref,
):
    s_peak, s_total, t_peak, t_total, cross = merged(stats_ref, Z)
    kl_ref[...] = cross / t_total - (t_peak + jnp.log(t_total)) + (s_peak + jnp.log(s_total))
    weight = stats_ref[0, 5:6]
    rows = [s_peak, weight / s_total, t_peak, weight / t_total, jnp.zeros((124, TOK), F32)]
    table = jnp.concatenate(rows, axis=0).T
    for n in range(VOC // TILE):
        s_by = jnp.exp(s_tile_ref[n] - table[:, 0:1]) * table[:, 1:2]
        t_by = jnp.exp(t_tile_ref[n] - table[:, 2:3]) * table[:, 3:4]
        for c in range(n * TILE, (n + 1) * TILE, 128):
            cols = slice(c, c + 128)
            slopes_ref[:, cols] = (
                student_ref[:, cols] * s_by - teacher_ref[:, cols] * t_by
            ).astype(BF16)
    out_ref[...] = lax.dot_general(
        head_ref[...], slopes_ref[...], (((1,), (1,)), ((), ())), preferred_element_type=F32
    ).astype(BF16)


def first_backward(place, stats, student_exp, teacher_exp, s_tile, t_tile, head):
    rows = D // X
    values = (stats, student_exp, teacher_exp, s_tile, t_tile)
    return pl.pallas_call(
        first_backward_kernel,
        grid_spec=pltpu.PrefetchScalarGridSpec(
            num_scalar_prefetch=1,
            grid=(1,),
            in_specs=[whole(v.shape) for v in values]
            + [pl.BlockSpec((rows, VOC), lambda n, place: (lax.rem(place[0] + 2, X), 0))],
            out_specs=[whole((TOK, VOC)), whole((rows, TOK)), whole((1, TOK))],
        ),
        out_shape=[
            jax.ShapeDtypeStruct((TOK, VOC), BF16),
            jax.ShapeDtypeStruct((rows, TOK), BF16),
            jax.ShapeDtypeStruct((1, TOK), F32),
        ],
        compiler_params=pltpu.CompilerParams(vmem_limit_bytes=BACKWARD_LIMIT << 20),
        cost_estimate=pl.CostEstimate(
            flops=2 * TOK * rows * VOC, bytes_accessed=12 << 20, transcendentals=0
        ),
        name="first_backward",
    )(place, *values, head)


def rest_backward_kernel(place, slopes_ref, head_ref, out_ref):
    out_ref[0] = lax.dot_general(
        head_ref[...],
        slopes_ref[...],
        (((1,), (1,)), ((), ())),
        preferred_element_type=F32,
    ).astype(BF16)


def rest_backward(place, slopes, head):
    rows, cut = D // X, 1
    tall = rows // cut

    def head_at(n, place):
        turn = lax.rem(2 * lax.div(n, cut) + 1, 5)
        return (lax.rem(place[0] + turn, X) * cut + lax.rem(n, cut), 0)

    return pl.pallas_call(
        rest_backward_kernel,
        grid_spec=pltpu.PrefetchScalarGridSpec(
            num_scalar_prefetch=1,
            grid=(3 * cut,),
            in_specs=[whole((TOK, VOC)), pl.BlockSpec((tall, VOC), head_at)],
            out_specs=pl.BlockSpec((1, tall, TOK), lambda n, _: (lax.div(n, cut), lax.rem(n, cut), 0)),
        ),
        out_shape=jax.ShapeDtypeStruct((3, rows, TOK), BF16),
        compiler_params=pltpu.CompilerParams(vmem_limit_bytes=4 << 20),
        cost_estimate=pl.CostEstimate(
            flops=6 * TOK * rows * VOC, bytes_accessed=10 << 20, transcendentals=0
        ),
        name="rest_backward",
    )(place, slopes, head)


def sum_kernel(pieces_ref, out_ref):
    out_ref[...] = sum(pieces_ref[k].astype(F32) for k in range(Z)).astype(BF16)


def reduced(far, prev_next_own):
    half = far.shape[0] // 2
    from_prev, from_next = shifted(far[:half], "x", 1), shifted(far[half:], "x", -1)
    to_next, to_prev, own = prev_next_own
    wide = lambda v: v.astype(F32)
    up = jnp.concatenate([(wide(to_next[:half]) + wide(from_prev)).astype(BF16), to_next[half:]])
    down = jnp.concatenate([to_prev[:half], (wide(to_prev[half:]) + wide(from_next)).astype(BF16)])
    total = wide(own) + wide(shifted(up, "x", 1)) + wide(shifted(down, "x", -1))
    pieces = total.astype(BF16).reshape(Z, FEAT, TOK)
    pieces = lax.all_to_all(pieces, "z", split_axis=0, concat_axis=0, tiled=True)
    (done,) = local(sum_kernel, [((FEAT, TOK), BF16)], 4, "sum_z", pieces)
    return done


def per_device(student_hidden, teacher_hidden, head, mask, steps):
    row = mask.reshape(1, TOK)
    half, block = (HALF, 2 * FEAT), (8, 128)
    here = jnp.stack([lax.axis_index("x"), lax.axis_index("z")]).astype(jnp.int32)
    place = jnp.concatenate([here, steps])
    a, b, count = local(
        entry_kernel, [(half, BF16), ((Z, *half), BF16), (block, F32)], 56, "entry",
        student_hidden.T, teacher_hidden.T, row,
    )
    parts, place, count, head = gathered(place, a, b, count, head)
    student_exp, teacher_exp, stats, s_tile, t_tile = forward(place, parts, count, row, head)
    stats = exchanged(stats, "x")
    (stats,) = local(merge_kernel, [((Z, 8, TOK), F32)], 4, "merge_x", stats)
    stats = exchanged(stats, "z")
    slopes, far, divergence = first_backward(
        place, stats, student_exp, teacher_exp, s_tile, t_tile, head
    )
    rest = rest_backward(place, slopes, head)
    summed = reduced(far, rest)
    return (divergence[0], summed.T)


def solution(mesh):
    torus = Mesh(mesh.devices.reshape(mesh.shape["dp"], X, Z), ("dp", "x", "z"))
    split = ("x", "z")
    in_specs = (P("dp", split), P("dp", split), P(None, split), P("dp"), P("dp"))
    out_specs = (P("dp"), P("dp", split))
    return jax.shard_map(
        per_device, mesh=torus, in_specs=in_specs, out_specs=out_specs, check_vma=False
    )
```

```python
import functools

import jax
import jax.numpy as jnp
from jax import lax
from jax.experimental import pallas as pl
from jax.experimental.pallas import tpu as pltpu
from jax.sharding import Mesh
from jax.sharding import PartitionSpec as P

LENGTH = 128
STEPS = 8
X, Z = 4, 8
TOK = 512
HALF = 256
FEAT = 64
D = 2048
VOC = 2048
TILE = 512
FORWARD_LIMIT = 22
LINES = 24
BACKWARD_LIMIT = 24
RESIDENT_LIMIT = 44
F32 = jnp.float32
BF16 = jnp.bfloat16


def shifted(value, axis, step):
    size = X if axis == "x" else Z
    return lax.ppermute(value, axis, [(i, (i + step) % size) for i in range(size)])


def exchanged(value, axis):
    return lax.all_to_all(value, axis, split_axis=0, concat_axis=0, tiled=True)


def local(kernel, shapes, limit, name, *values):
    return pl.pallas_call(
        kernel,
        out_shape=[jax.ShapeDtypeStruct(shape, kind) for shape, kind in shapes],
        compiler_params=pltpu.CompilerParams(vmem_limit_bytes=limit << 20),
        name=name,
    )(*values)


def entry_kernel(student_ref, teacher_ref, mask_ref, a_ref, b_ref, count_ref):
    both = jnp.concatenate([student_ref[...], teacher_ref[...]], axis=0).T
    a_ref[...] = both[:HALF]
    b_ref[...] = jnp.broadcast_to(both[HALF:], b_ref.shape)
    count_ref[...] = jnp.full((8, 128), jnp.sum(mask_ref[...].astype(F32)))


def side_by_side(blocks, out_ref):
    for lanes, rows in ((slice(0, FEAT), slice(0, HALF)), (slice(FEAT, None), slice(HALF, None))):
        out_ref[rows] = jnp.concatenate([block[:, lanes] for block in blocks], axis=1)


def pack_a_kernel(*refs):
    side_by_side([ref[...] for ref in refs[:-1]], refs[-1])


def pack_b_kernel(place_ref, blocks_ref, out_ref):
    side_by_side([blocks_ref[lax.rem(place_ref[1] + k, Z)] for k in range(Z)], out_ref)


def pack_b(place, blocks):
    return pl.pallas_call(
        pack_b_kernel,
        in_specs=[pl.BlockSpec(memory_space=pltpu.SMEM), pl.BlockSpec(memory_space=pltpu.VMEM)],
        out_shape=jax.ShapeDtypeStruct((2 * HALF, Z * FEAT), BF16),
        compiler_params=pltpu.CompilerParams(vmem_limit_bytes=4 << 20),
        name="pack_b",
    )(place, blocks)


def tied(*values):
    return lax.optimization_barrier(values)


def added_over_dp(count, bit):
    pairs = [(i, i ^ bit) for i in range(lax.axis_size("dp"))]
    return count + lax.ppermute(count, "dp", pairs)


def gathered(place, a, b, count, head):
    a_next, a_prev, a_far = shifted(a, "x", -1), shifted(a, "x", 1), shifted(a, "x", 2)
    b = exchanged(b, "z")
    a_next, place = tied(a_next, place)
    packed = [((2 * HALF, X * FEAT), BF16)]
    (own_a,) = local(pack_a_kernel, packed, 4, "pack_a", a, a_next, a_far, a_prev)
    own_b, head, count = tied(pack_b(place, b), head, added_over_dp(count, 1))
    head = resident(head)
    ahead, behind = [own_a], [own_a]
    for hop in range(3):
        if hop == 2:
            count = added_over_dp(count, 2)
            behind[-1], ahead[-1], count, head = tied(behind[-1], ahead[-1], count, head)
        behind.append(shifted(behind[-1], "z", 1))
        ahead.append(shifted(ahead[-1], "z", -1))
    behind[-1], ahead[-1], count = tied(behind[-1], ahead[-1], added_over_dp(count, 4))
    low, high = shifted(behind[-1][:HALF], "z", 1), shifted(ahead[-1][HALF:], "z", -1)
    b_prev, b_next = shifted(own_b, "x", 1), shifted(own_b, "x", -1)
    far_low, far_high = shifted(b_prev[:HALF], "x", 1), shifted(b_next[HALF:], "x", -1)
    return (*ahead, low, high, *behind[:0:-1], own_b, b_next, far_low, far_high, b_prev), place, count, head


def resident_kernel(head_ref, out_ref, done):
    copy = pltpu.make_async_copy(head_ref, out_ref, done)
    copy.start()
    copy.wait()


def resident(head):
    return pl.pallas_call(
        resident_kernel,
        in_specs=[pl.BlockSpec(memory_space=pl.ANY)],
        out_specs=pl.BlockSpec(memory_space=pltpu.VMEM),
        out_shape=jax.ShapeDtypeStruct(head.shape, head.dtype),
        scratch_shapes=[pltpu.SemaphoreType.DMA],
        compiler_params=pltpu.CompilerParams(vmem_limit_bytes=RESIDENT_LIMIT << 20),
        cost_estimate=pl.CostEstimate(flops=3 << 30, bytes_accessed=16 << 20, transcendentals=0),
        name="resident",
    )(head)


def whole(shape):
    return pl.BlockSpec(shape, lambda *_: (0,) * len(shape))


def interleaved(pieces, rows_ref):
    lane = lax.broadcasted_iota(jnp.int32, (2 * HALF, 128), 1)
    for pair in range(Z // 2):
        tiles = [piece[:, pair * 128 : pair * 128 + 128] for piece in pieces]
        turned = [jnp.concatenate([t[:, FEAT:], t[:, :FEAT]], axis=1) for t in tiles]
        for side, (lower, upper) in enumerate(((tiles, turned), (turned, tiles))):
            at = (2 * pair + side) * X * FEAT
            for i in range(0, X, 2):
                both = jnp.where(lane < FEAT, lower[i], upper[i + 1])
                rows_ref[2 * HALF :, at + i * FEAT : at + i * FEAT + 128] = both


def tile_stats(student_ref, teacher_ref, n, state):
    cols = [slice(c, c + 128) for c in range(n * TILE, (n + 1) * TILE, 128)]
    s_old, s_total, t_old, t_total, cross = state
    s_peak = functools.reduce(jnp.maximum, [student_ref[:, c] for c in cols], s_old)
    t_peak = functools.reduce(jnp.maximum, [teacher_ref[:, c] for c in cols], t_old)
    s_total = s_total * jnp.exp(s_old - s_peak)
    t_scale = jnp.exp(t_old - t_peak)
    t_total, cross = t_total * t_scale, cross * t_scale
    for c in cols:
        s_part, t_part = student_ref[:, c], teacher_ref[:, c]
        s_exp, t_exp = jnp.exp(s_part - s_peak), jnp.exp(t_part - t_peak)
        s_total += s_exp
        t_total += t_exp
        cross += t_exp * (t_part - s_part)
        student_ref[:, c] = s_exp
        teacher_ref[:, c] = t_exp
    return s_peak, s_total, t_peak, t_total, cross


def forward_kernel(place, *refs):
    a_refs, b_refs = refs[:9], refs[9:14]
    count_ref, mask_ref, head_ref, student_ref, teacher_ref = refs[14:19]
    stats_ref, weight_ref, s_tile_ref, t_tile_ref, state_ref, rows_ref = refs[19:]
    x, z = place[0], place[1]
    width = X * FEAT
    for k, ref in enumerate((*a_refs[:4], None, *a_refs[6:])):
        if ref is not None:
            rows_ref[: 2 * HALF, k * width : (k + 1) * width] = ref[...]
    rows_ref[:HALF, 4 * width : 5 * width] = a_refs[4][...]
    rows_ref[HALF : 2 * HALF, 4 * width : 5 * width] = a_refs[5][...]
    b_far = jnp.concatenate([b_refs[2][...], b_refs[3][...]], axis=0)
    interleaved([b_refs[0][...], b_refs[1][...], b_far, b_refs[4][...]], rows_ref)

    def multiply(n):
        cols = slice(n * TILE, (n + 1) * TILE)
        weights = [
            head_ref[lax.rem(x + i, X), lax.rem(z + k, Z), :, cols]
            for k in range(Z)
            for i in range(X)
        ]
        logs = jnp.dot(rows_ref[...], jnp.concatenate(weights, axis=0), preferred_element_type=F32)
        student_ref[:HALF, cols] = logs[:HALF]
        teacher_ref[:HALF, cols] = logs[HALF : 2 * HALF]
        student_ref[HALF:, cols] = logs[2 * HALF : 3 * HALF]
        teacher_ref[HALF:, cols] = logs[3 * HALF :]

    def summarize(n):
        if n:
            state = [state_ref[row] for row in range(5)]
        else:
            low, zero = jnp.full((TOK, 128), -jnp.inf, F32), jnp.zeros((TOK, 128), F32)
            state = [low, zero, low, zero, zero]
        state = tile_stats(student_ref, teacher_ref, n, state)
        for row, value in enumerate(state):
            state_ref[row] = value
        s_tile_ref[n], t_tile_ref[n] = state[0], state[2]

    tiles = VOC // TILE
    for n in range(tiles + 1):
        if n < tiles:
            multiply(n)
        if n:
            summarize(n - 1)

    s_peak, s_total, t_peak, t_total, cross = [state_ref[row] for row in range(5)]
    s_top = jnp.max(s_peak, axis=1, keepdims=True)
    t_top = jnp.max(t_peak, axis=1, keepdims=True)
    s_by, t_by = jnp.exp(s_peak - s_top), jnp.exp(t_peak - t_top)
    columns = [
        s_top,
        jnp.sum(s_total * s_by, axis=1, keepdims=True),
        t_top,
        jnp.sum(t_total * t_by, axis=1, keepdims=True),
        jnp.sum(cross * t_by, axis=1, keepdims=True),
    ]
    lane = lax.broadcasted_iota(jnp.int32, (TOK, 128), 1)
    table = jnp.zeros((TOK, 128), F32)
    for k, column in enumerate(columns):
        table = jnp.where(lane == k, column, table)
    token = lax.broadcasted_iota(jnp.int32, (1, TOK), 1)
    steps = jnp.full((1, TOK), place[2])
    for k in range(1, TOK // LENGTH):
        steps = jnp.where(token >= k * LENGTH, place[2 + k], steps)
    factor = STEPS / steps.astype(F32)
    scale = float(8 * TOK) / jnp.maximum(count_ref[0:1, 0:1], 1.0)
    weight = mask_ref[...].astype(F32) * factor * scale
    weight_ref[...] = weight
    rows = table.T[:8]
    lines = [rows[k : k + 1, c : c + 128] for k in range(5) for c in range(0, TOK, 128)]
    block = jnp.concatenate([*lines, jnp.zeros((LINES - len(lines), 128), F32)], axis=0)
    stats_ref[...] = jnp.broadcast_to(block, (X * Z, LINES, 128))


def forward(place, parts, count, mask, head):
    values = (*parts, count, mask)
    tiles = VOC // TILE
    logs = jax.ShapeDtypeStruct((TOK, VOC), F32)
    peaks = jax.ShapeDtypeStruct((tiles, TOK, 128), F32)
    return pl.pallas_call(
        forward_kernel,
        grid_spec=pltpu.PrefetchScalarGridSpec(
            num_scalar_prefetch=1,
            grid=(1,),
            in_specs=[whole(v.shape) for v in values]
            + [whole((X, Z, FEAT, VOC))],
            out_specs=[
                whole((TOK, VOC)),
                whole((TOK, VOC)),
                whole((X * Z, LINES, 128)),
                whole((1, TOK)),
                whole((tiles, TOK, 128)),
                whole((tiles, TOK, 128)),
            ],
            scratch_shapes=[pltpu.VMEM((5, TOK, 128), F32), pltpu.VMEM((4 * HALF, D), BF16)],
        ),
        out_shape=[
            logs,
            logs,
            jax.ShapeDtypeStruct((X * Z, LINES, 128), F32),
            jax.ShapeDtypeStruct((1, TOK), F32),
            peaks,
            peaks,
        ],
        compiler_params=pltpu.CompilerParams(vmem_limit_bytes=FORWARD_LIMIT << 20),
        cost_estimate=pl.CostEstimate(
            flops=4 * TOK * D * VOC, bytes_accessed=4 << 20, transcendentals=0
        ),
        name="forward",
    )(place, *values, head.reshape(X, Z, FEAT, VOC))


def merged(stats_ref, count):
    high = TOK // 128
    rows = [[stats_ref[k, row * high : (row + 1) * high] for k in range(count)] for row in range(5)]
    s_peak = functools.reduce(jnp.maximum, rows[0])
    t_peak = functools.reduce(jnp.maximum, rows[2])
    s_by = [jnp.exp(peak - s_peak) for peak in rows[0]]
    t_by = [jnp.exp(peak - t_peak) for peak in rows[2]]
    s_total = sum(total * by for total, by in zip(rows[1], s_by))
    t_total = sum(total * by for total, by in zip(rows[3], t_by))
    cross = sum(total * by for total, by in zip(rows[4], t_by))
    found = (s_peak, s_total, t_peak, t_total, cross)
    return [jnp.concatenate([v[k : k + 1] for k in range(high)], axis=1) for v in found]


def first_backward_kernel(
    place, stats_ref, weight_ref, student_ref, teacher_ref, s_tile_ref, t_tile_ref, head_ref,
    slopes_ref, out_ref, kl_ref,
):
    s_peak, s_total, t_peak, t_total, cross = merged(stats_ref, X * Z)
    kl_ref[...] = cross / t_total - (t_peak + jnp.log(t_total)) + (s_peak + jnp.log(s_total))
    weight = weight_ref[...]
    rows = [s_peak, weight / s_total, t_peak, weight / t_total, jnp.zeros((124, TOK), F32)]
    table = jnp.concatenate(rows, axis=0).T
    for n in range(VOC // TILE):
        s_by = jnp.exp(s_tile_ref[n] - table[:, 0:1]) * table[:, 1:2]
        t_by = jnp.exp(t_tile_ref[n] - table[:, 2:3]) * table[:, 3:4]
        for c in range(n * TILE, (n + 1) * TILE, 128):
            cols = slice(c, c + 128)
            slopes_ref[:, cols] = (
                student_ref[:, cols] * s_by - teacher_ref[:, cols] * t_by
            ).astype(BF16)
    out_ref[...] = lax.dot_general(
        head_ref[...], slopes_ref[...], (((1,), (1,)), ((), ())), preferred_element_type=F32
    ).astype(BF16)


def first_backward(place, stats, weight, student_exp, teacher_exp, s_tile, t_tile, head):
    rows = D // X
    values = (stats, weight, student_exp, teacher_exp, s_tile, t_tile)
    return pl.pallas_call(
        first_backward_kernel,
        grid_spec=pltpu.PrefetchScalarGridSpec(
            num_scalar_prefetch=1,
            grid=(1,),
            in_specs=[whole(v.shape) for v in values]
            + [pl.BlockSpec((rows, VOC), lambda n, place: (lax.rem(place[0] + 2, X), 0))],
            out_specs=[whole((TOK, VOC)), whole((rows, TOK)), whole((1, TOK))],
        ),
        out_shape=[
            jax.ShapeDtypeStruct((TOK, VOC), BF16),
            jax.ShapeDtypeStruct((rows, TOK), BF16),
            jax.ShapeDtypeStruct((1, TOK), F32),
        ],
        compiler_params=pltpu.CompilerParams(vmem_limit_bytes=BACKWARD_LIMIT << 20),
        cost_estimate=pl.CostEstimate(
            flops=2 * TOK * rows * VOC, bytes_accessed=12 << 20, transcendentals=0
        ),
        name="first_backward",
    )(place, *values, head)


def rest_backward_kernel(place, slopes_ref, head_ref, out_ref):
    out_ref[0] = lax.dot_general(
        head_ref[...],
        slopes_ref[...],
        (((1,), (1,)), ((), ())),
        preferred_element_type=F32,
    ).astype(BF16)


def rest_backward(place, slopes, head):
    rows, cut = D // X, 1
    tall = rows // cut

    def head_at(n, place):
        turn = lax.rem(2 * lax.div(n, cut) + 1, 5)
        return (lax.rem(place[0] + turn, X) * cut + lax.rem(n, cut), 0)

    return pl.pallas_call(
        rest_backward_kernel,
        grid_spec=pltpu.PrefetchScalarGridSpec(
            num_scalar_prefetch=1,
            grid=(3 * cut,),
            in_specs=[whole((TOK, VOC)), pl.BlockSpec((tall, VOC), head_at)],
            out_specs=pl.BlockSpec((1, tall, TOK), lambda n, _: (lax.div(n, cut), lax.rem(n, cut), 0)),
        ),
        out_shape=jax.ShapeDtypeStruct((3, rows, TOK), BF16),
        compiler_params=pltpu.CompilerParams(vmem_limit_bytes=4 << 20),
        cost_estimate=pl.CostEstimate(
            flops=6 * TOK * rows * VOC, bytes_accessed=10 << 20, transcendentals=0
        ),
        name="rest_backward",
    )(place, slopes, head)


def sum_kernel(pieces_ref, out_ref):
    out_ref[...] = sum(pieces_ref[k].astype(F32) for k in range(Z)).astype(BF16)


def reduced(far, prev_next_own):
    half = far.shape[0] // 2
    from_prev, from_next = shifted(far[:half], "x", 1), shifted(far[half:], "x", -1)
    to_next, to_prev, own = prev_next_own
    wide = lambda v: v.astype(F32)
    up = jnp.concatenate([(wide(to_next[:half]) + wide(from_prev)).astype(BF16), to_next[half:]])
    down = jnp.concatenate([to_prev[:half], (wide(to_prev[half:]) + wide(from_next)).astype(BF16)])
    total = wide(own) + wide(shifted(up, "x", 1)) + wide(shifted(down, "x", -1))
    pieces = total.astype(BF16).reshape(Z, FEAT, TOK)
    pieces = lax.all_to_all(pieces, "z", split_axis=0, concat_axis=0, tiled=True)
    (done,) = local(sum_kernel, [((FEAT, TOK), BF16)], 4, "sum_z", pieces)
    return done


def per_device(student_hidden, teacher_hidden, head, mask, steps):
    row = mask.reshape(1, TOK)
    half, block = (HALF, 2 * FEAT), (8, 128)
    here = jnp.stack([lax.axis_index("x"), lax.axis_index("z")]).astype(jnp.int32)
    place = jnp.concatenate([here, steps])
    a, b, count = local(
        entry_kernel, [(half, BF16), ((Z, *half), BF16), (block, F32)], 56, "entry",
        student_hidden.T, teacher_hidden.T, row,
    )
    parts, place, count, head = gathered(place, a, b, count, head)
    student_exp, teacher_exp, stats, weight, s_tile, t_tile = forward(place, parts, count, row, head)
    stats = exchanged(stats, ("x", "z"))
    slopes, far, divergence = first_backward(
        place, stats, weight, student_exp, teacher_exp, s_tile, t_tile, head
    )
    rest = rest_backward(place, slopes, head)
    summed = reduced(far, rest)
    return (divergence[0], summed.T)


def solution(mesh):
    torus = Mesh(mesh.devices.reshape(mesh.shape["dp"], X, Z), ("dp", "x", "z"))
    split = ("x", "z")
    in_specs = (P("dp", split), P("dp", split), P(None, split), P("dp"), P("dp"))
    out_specs = (P("dp"), P("dp", split))
    return jax.shard_map(
        per_device, mesh=torus, in_specs=in_specs, out_specs=out_specs, check_vma=False
    )
```

```python
import functools

import jax
import jax.numpy as jnp
from jax import lax
from jax.experimental import pallas as pl
from jax.experimental.pallas import tpu as pltpu
from jax.sharding import Mesh
from jax.sharding import PartitionSpec as P

LENGTH = 128
STEPS = 8
X, Z = 4, 8
TOK = 512
HALF = 256
FEAT = 64
D = 2048
VOC = 2048
TILE = 512
FORWARD_LIMIT = 22
LINES = 24
BACKWARD_LIMIT = 24
RESIDENT_LIMIT = 44
F32 = jnp.float32
BF16 = jnp.bfloat16


def shifted(value, axis, step):
    size = X if axis == "x" else Z
    return lax.ppermute(value, axis, [(i, (i + step) % size) for i in range(size)])


def exchanged(value, axis):
    return lax.all_to_all(value, axis, split_axis=0, concat_axis=0, tiled=True)


def local(kernel, shapes, limit, name, *values):
    return pl.pallas_call(
        kernel,
        out_shape=[jax.ShapeDtypeStruct(shape, kind) for shape, kind in shapes],
        compiler_params=pltpu.CompilerParams(vmem_limit_bytes=limit << 20),
        name=name,
    )(*values)


def entry_kernel(student_ref, teacher_ref, mask_ref, a_ref, b_ref, count_ref):
    both = jnp.concatenate([student_ref[...], teacher_ref[...]], axis=0).T
    a_ref[...] = both[:HALF]
    b_ref[...] = jnp.broadcast_to(both[HALF:], b_ref.shape)
    count_ref[...] = jnp.full((8, 128), jnp.sum(mask_ref[...].astype(F32)))


def side_by_side(blocks, out_ref):
    for lanes, rows in ((slice(0, FEAT), slice(0, HALF)), (slice(FEAT, None), slice(HALF, None))):
        out_ref[rows] = jnp.concatenate([block[:, lanes] for block in blocks], axis=1)


def pack_a_kernel(*refs):
    side_by_side([ref[...] for ref in refs[:-1]], refs[-1])


def pack_b_kernel(place_ref, blocks_ref, out_ref):
    side_by_side([blocks_ref[lax.rem(place_ref[1] + k, Z)] for k in range(Z)], out_ref)


def pack_b(place, blocks):
    return pl.pallas_call(
        pack_b_kernel,
        in_specs=[pl.BlockSpec(memory_space=pltpu.SMEM), pl.BlockSpec(memory_space=pltpu.VMEM)],
        out_shape=jax.ShapeDtypeStruct((2 * HALF, Z * FEAT), BF16),
        compiler_params=pltpu.CompilerParams(vmem_limit_bytes=4 << 20),
        name="pack_b",
    )(place, blocks)


def tied(*values):
    return lax.optimization_barrier(values)


def added_over_dp(count, bit):
    pairs = [(i, i ^ bit) for i in range(lax.axis_size("dp"))]
    return count + lax.ppermute(count, "dp", pairs)


def gathered(place, a, b, count, head):
    a_next, a_prev, a_far = shifted(a, "x", -1), shifted(a, "x", 1), shifted(a, "x", 2)
    b = exchanged(b, "z")
    a_next, place = tied(a_next, place)
    packed = [((2 * HALF, X * FEAT), BF16)]
    (own_a,) = local(pack_a_kernel, packed, 4, "pack_a", a, a_next, a_far, a_prev)
    own_b, head, count = tied(pack_b(place, b), head, added_over_dp(count, 1))
    head = resident(head)
    ahead, behind = [own_a], [own_a]
    for hop in range(3):
        if hop == 2:
            count = added_over_dp(count, 2)
            behind[-1], ahead[-1], count, head = tied(behind[-1], ahead[-1], count, head)
        behind.append(shifted(behind[-1], "z", 1))
        ahead.append(shifted(ahead[-1], "z", -1))
    low, high = shifted(behind[-1][:HALF], "z", 1), shifted(ahead[-1][HALF:], "z", -1)
    count = added_over_dp(count, 4)
    b_prev, b_next = shifted(own_b, "x", 1), shifted(own_b, "x", -1)
    far_low, far_high = shifted(b_prev[:HALF], "x", 1), shifted(b_next[HALF:], "x", -1)
    return (*ahead, low, high, *behind[:0:-1], own_b, b_next, far_low, far_high, b_prev), place, count, head


def resident_kernel(head_ref, out_ref, done):
    copy = pltpu.make_async_copy(head_ref, out_ref, done)
    copy.start()
    copy.wait()


def resident(head):
    return pl.pallas_call(
        resident_kernel,
        in_specs=[pl.BlockSpec(memory_space=pl.ANY)],
        out_specs=pl.BlockSpec(memory_space=pltpu.VMEM),
        out_shape=jax.ShapeDtypeStruct(head.shape, head.dtype),
        scratch_shapes=[pltpu.SemaphoreType.DMA],
        compiler_params=pltpu.CompilerParams(vmem_limit_bytes=RESIDENT_LIMIT << 20),
        cost_estimate=pl.CostEstimate(flops=3 << 30, bytes_accessed=16 << 20, transcendentals=0),
        name="resident",
    )(head)


def whole(shape):
    return pl.BlockSpec(shape, lambda *_: (0,) * len(shape))


def interleaved(pieces, rows_ref):
    lane = lax.broadcasted_iota(jnp.int32, (2 * HALF, 128), 1)
    for pair in range(Z // 2):
        tiles = [piece[:, pair * 128 : pair * 128 + 128] for piece in pieces]
        turned = [jnp.concatenate([t[:, FEAT:], t[:, :FEAT]], axis=1) for t in tiles]
        for side, (lower, upper) in enumerate(((tiles, turned), (turned, tiles))):
            at = (2 * pair + side) * X * FEAT
            for i in range(0, X, 2):
                both = jnp.where(lane < FEAT, lower[i], upper[i + 1])
                rows_ref[2 * HALF :, at + i * FEAT : at + i * FEAT + 128] = both


def tile_stats(student_ref, teacher_ref, n, state):
    cols = [slice(c, c + 128) for c in range(n * TILE, (n + 1) * TILE, 128)]
    s_old, s_total, t_old, t_total, cross = state
    s_peak = functools.reduce(jnp.maximum, [student_ref[:, c] for c in cols], s_old)
    t_peak = functools.reduce(jnp.maximum, [teacher_ref[:, c] for c in cols], t_old)
    s_total = s_total * jnp.exp(s_old - s_peak)
    t_scale = jnp.exp(t_old - t_peak)
    t_total, cross = t_total * t_scale, cross * t_scale
    for c in cols:
        s_part, t_part = student_ref[:, c], teacher_ref[:, c]
        s_exp, t_exp = jnp.exp(s_part - s_peak), jnp.exp(t_part - t_peak)
        s_total += s_exp
        t_total += t_exp
        cross += t_exp * (t_part - s_part)
        student_ref[:, c] = s_exp
        teacher_ref[:, c] = t_exp
    return s_peak, s_total, t_peak, t_total, cross


def forward_kernel(place, *refs):
    a_refs, b_refs = refs[:9], refs[9:14]
    count_ref, mask_ref, head_ref, student_ref, teacher_ref = refs[14:19]
    stats_ref, weight_ref, s_tile_ref, t_tile_ref, state_ref, rows_ref = refs[19:]
    x, z = place[0], place[1]
    width = X * FEAT
    for k, ref in enumerate((*a_refs[:4], None, *a_refs[6:])):
        if ref is not None:
            rows_ref[: 2 * HALF, k * width : (k + 1) * width] = ref[...]
    rows_ref[:HALF, 4 * width : 5 * width] = a_refs[4][...]
    rows_ref[HALF : 2 * HALF, 4 * width : 5 * width] = a_refs[5][...]
    b_far = jnp.concatenate([b_refs[2][...], b_refs[3][...]], axis=0)
    interleaved([b_refs[0][...], b_refs[1][...], b_far, b_refs[4][...]], rows_ref)

    def multiply(n):
        cols = slice(n * TILE, (n + 1) * TILE)
        weights = [
            head_ref[lax.rem(x + i, X), lax.rem(z + k, Z), :, cols]
            for k in range(Z)
            for i in range(X)
        ]
        logs = jnp.dot(rows_ref[...], jnp.concatenate(weights, axis=0), preferred_element_type=F32)
        student_ref[:HALF, cols] = logs[:HALF]
        teacher_ref[:HALF, cols] = logs[HALF : 2 * HALF]
        student_ref[HALF:, cols] = logs[2 * HALF : 3 * HALF]
        teacher_ref[HALF:, cols] = logs[3 * HALF :]

    def summarize(n):
        if n:
            state = [state_ref[row] for row in range(5)]
        else:
            low, zero = jnp.full((TOK, 128), -jnp.inf, F32), jnp.zeros((TOK, 128), F32)
            state = [low, zero, low, zero, zero]
        state = tile_stats(student_ref, teacher_ref, n, state)
        for row, value in enumerate(state):
            state_ref[row] = value
        s_tile_ref[n], t_tile_ref[n] = state[0], state[2]

    tiles = VOC // TILE
    for n in range(tiles + 1):
        if n < tiles:
            multiply(n)
        if n:
            summarize(n - 1)

    s_peak, s_total, t_peak, t_total, cross = [state_ref[row] for row in range(5)]
    s_top = jnp.max(s_peak, axis=1, keepdims=True)
    t_top = jnp.max(t_peak, axis=1, keepdims=True)
    s_by, t_by = jnp.exp(s_peak - s_top), jnp.exp(t_peak - t_top)
    columns = [
        s_top,
        jnp.sum(s_total * s_by, axis=1, keepdims=True),
        t_top,
        jnp.sum(t_total * t_by, axis=1, keepdims=True),
        jnp.sum(cross * t_by, axis=1, keepdims=True),
    ]
    lane = lax.broadcasted_iota(jnp.int32, (TOK, 128), 1)
    table = jnp.zeros((TOK, 128), F32)
    for k, column in enumerate(columns):
        table = jnp.where(lane == k, column, table)
    token = lax.broadcasted_iota(jnp.int32, (1, TOK), 1)
    steps = jnp.full((1, TOK), place[2])
    for k in range(1, TOK // LENGTH):
        steps = jnp.where(token >= k * LENGTH, place[2 + k], steps)
    factor = STEPS / steps.astype(F32)
    scale = float(8 * TOK) / jnp.maximum(count_ref[0:1, 0:1], 1.0)
    weight = mask_ref[...].astype(F32) * factor * scale
    weight_ref[...] = weight
    rows = table.T[:8]
    lines = [rows[k : k + 1, c : c + 128] for k in range(5) for c in range(0, TOK, 128)]
    block = jnp.concatenate([*lines, jnp.zeros((LINES - len(lines), 128), F32)], axis=0)
    stats_ref[...] = jnp.broadcast_to(block, (X * Z, LINES, 128))


def forward(place, parts, count, mask, head):
    values = (*parts, count, mask)
    tiles = VOC // TILE
    logs = jax.ShapeDtypeStruct((TOK, VOC), F32)
    peaks = jax.ShapeDtypeStruct((tiles, TOK, 128), F32)
    return pl.pallas_call(
        forward_kernel,
        grid_spec=pltpu.PrefetchScalarGridSpec(
            num_scalar_prefetch=1,
            grid=(1,),
            in_specs=[whole(v.shape) for v in values]
            + [whole((X, Z, FEAT, VOC))],
            out_specs=[
                whole((TOK, VOC)),
                whole((TOK, VOC)),
                whole((X * Z, LINES, 128)),
                whole((1, TOK)),
                whole((tiles, TOK, 128)),
                whole((tiles, TOK, 128)),
            ],
            scratch_shapes=[pltpu.VMEM((5, TOK, 128), F32), pltpu.VMEM((4 * HALF, D), BF16)],
        ),
        out_shape=[
            logs,
            logs,
            jax.ShapeDtypeStruct((X * Z, LINES, 128), F32),
            jax.ShapeDtypeStruct((1, TOK), F32),
            peaks,
            peaks,
        ],
        compiler_params=pltpu.CompilerParams(vmem_limit_bytes=FORWARD_LIMIT << 20),
        cost_estimate=pl.CostEstimate(
            flops=4 * TOK * D * VOC, bytes_accessed=4 << 20, transcendentals=0
        ),
        name="forward",
    )(place, *values, head.reshape(X, Z, FEAT, VOC))


def merged(stats_ref, count):
    high = TOK // 128
    rows = [[stats_ref[k, row * high : (row + 1) * high] for k in range(count)] for row in range(5)]
    s_peak = functools.reduce(jnp.maximum, rows[0])
    t_peak = functools.reduce(jnp.maximum, rows[2])
    s_by = [jnp.exp(peak - s_peak) for peak in rows[0]]
    t_by = [jnp.exp(peak - t_peak) for peak in rows[2]]
    s_total = sum(total * by for total, by in zip(rows[1], s_by))
    t_total = sum(total * by for total, by in zip(rows[3], t_by))
    cross = sum(total * by for total, by in zip(rows[4], t_by))
    found = (s_peak, s_total, t_peak, t_total, cross)
    return [jnp.concatenate([v[k : k + 1] for k in range(high)], axis=1) for v in found]


def first_backward_kernel(
    place, stats_ref, weight_ref, student_ref, teacher_ref, s_tile_ref, t_tile_ref, head_ref,
    slopes_ref, out_ref, kl_ref,
):
    s_peak, s_total, t_peak, t_total, cross = merged(stats_ref, X * Z)
    kl_ref[...] = cross / t_total - (t_peak + jnp.log(t_total)) + (s_peak + jnp.log(s_total))
    weight = weight_ref[...]
    rows = [s_peak, weight / s_total, t_peak, weight / t_total, jnp.zeros((124, TOK), F32)]
    table = jnp.concatenate(rows, axis=0).T
    for n in range(VOC // TILE):
        s_by = jnp.exp(s_tile_ref[n] - table[:, 0:1]) * table[:, 1:2]
        t_by = jnp.exp(t_tile_ref[n] - table[:, 2:3]) * table[:, 3:4]
        for c in range(n * TILE, (n + 1) * TILE, 128):
            cols = slice(c, c + 128)
            slopes_ref[:, cols] = (
                student_ref[:, cols] * s_by - teacher_ref[:, cols] * t_by
            ).astype(BF16)
    out_ref[...] = lax.dot_general(
        head_ref[...], slopes_ref[...], (((1,), (1,)), ((), ())), preferred_element_type=F32
    ).astype(BF16)


def first_backward(place, stats, weight, student_exp, teacher_exp, s_tile, t_tile, head):
    rows = D // X
    values = (stats, weight, student_exp, teacher_exp, s_tile, t_tile)
    return pl.pallas_call(
        first_backward_kernel,
        grid_spec=pltpu.PrefetchScalarGridSpec(
            num_scalar_prefetch=1,
            grid=(1,),
            in_specs=[whole(v.shape) for v in values]
            + [pl.BlockSpec((rows, VOC), lambda n, place: (lax.rem(place[0] + 2, X), 0))],
            out_specs=[whole((TOK, VOC)), whole((rows, TOK)), whole((1, TOK))],
        ),
        out_shape=[
            jax.ShapeDtypeStruct((TOK, VOC), BF16),
            jax.ShapeDtypeStruct((rows, TOK), BF16),
            jax.ShapeDtypeStruct((1, TOK), F32),
        ],
        compiler_params=pltpu.CompilerParams(vmem_limit_bytes=BACKWARD_LIMIT << 20),
        cost_estimate=pl.CostEstimate(
            flops=2 * TOK * rows * VOC, bytes_accessed=12 << 20, transcendentals=0
        ),
        name="first_backward",
    )(place, *values, head)


def rest_backward_kernel(place, slopes_ref, head_ref, out_ref):
    out_ref[0] = lax.dot_general(
        head_ref[...],
        slopes_ref[...],
        (((1,), (1,)), ((), ())),
        preferred_element_type=F32,
    ).astype(BF16)


def rest_backward(place, slopes, head):
    rows, cut = D // X, 1
    tall = rows // cut

    def head_at(n, place):
        turn = lax.rem(2 * lax.div(n, cut) + 1, 5)
        return (lax.rem(place[0] + turn, X) * cut + lax.rem(n, cut), 0)

    return pl.pallas_call(
        rest_backward_kernel,
        grid_spec=pltpu.PrefetchScalarGridSpec(
            num_scalar_prefetch=1,
            grid=(3 * cut,),
            in_specs=[whole((TOK, VOC)), pl.BlockSpec((tall, VOC), head_at)],
            out_specs=pl.BlockSpec((1, tall, TOK), lambda n, _: (lax.div(n, cut), lax.rem(n, cut), 0)),
        ),
        out_shape=jax.ShapeDtypeStruct((3, rows, TOK), BF16),
        compiler_params=pltpu.CompilerParams(vmem_limit_bytes=4 << 20),
        cost_estimate=pl.CostEstimate(
            flops=6 * TOK * rows * VOC, bytes_accessed=10 << 20, transcendentals=0
        ),
        name="rest_backward",
    )(place, slopes, head)


def sum_kernel(pieces_ref, out_ref):
    out_ref[...] = sum(pieces_ref[k].astype(F32) for k in range(Z)).astype(BF16)


def reduced(far, prev_next_own):
    half = far.shape[0] // 2
    from_prev, from_next = shifted(far[:half], "x", 1), shifted(far[half:], "x", -1)
    to_next, to_prev, own = prev_next_own
    wide = lambda v: v.astype(F32)
    up = jnp.concatenate([(wide(to_next[:half]) + wide(from_prev)).astype(BF16), to_next[half:]])
    down = jnp.concatenate([to_prev[:half], (wide(to_prev[half:]) + wide(from_next)).astype(BF16)])
    total = wide(own) + wide(shifted(up, "x", 1)) + wide(shifted(down, "x", -1))
    pieces = total.astype(BF16).reshape(Z, FEAT, TOK)
    pieces = lax.all_to_all(pieces, "z", split_axis=0, concat_axis=0, tiled=True)
    (done,) = local(sum_kernel, [((FEAT, TOK), BF16)], 4, "sum_z", pieces)
    return done


def per_device(student_hidden, teacher_hidden, head, mask, steps):
    row = mask.reshape(1, TOK)
    half, block = (HALF, 2 * FEAT), (8, 128)
    here = jnp.stack([lax.axis_index("x"), lax.axis_index("z")]).astype(jnp.int32)
    place = jnp.concatenate([here, steps])
    a, b, count = local(
        entry_kernel, [(half, BF16), ((Z, *half), BF16), (block, F32)], 56, "entry",
        student_hidden.T, teacher_hidden.T, row,
    )
    parts, place, count, head = gathered(place, a, b, count, head)
    student_exp, teacher_exp, stats, weight, s_tile, t_tile = forward(place, parts, count, row, head)
    stats = exchanged(stats, ("x", "z"))
    slopes, far, divergence = first_backward(
        place, stats, weight, student_exp, teacher_exp, s_tile, t_tile, head
    )
    rest = rest_backward(place, slopes, head)
    summed = reduced(far, rest)
    return (divergence[0], summed.T)


def solution(mesh):
    torus = Mesh(mesh.devices.reshape(mesh.shape["dp"], X, Z), ("dp", "x", "z"))
    split = ("x", "z")
    in_specs = (P("dp", split), P("dp", split), P(None, split), P("dp"), P("dp"))
    out_specs = (P("dp"), P("dp", split))
    return jax.shard_map(
        per_device, mesh=torus, in_specs=in_specs, out_specs=out_specs, check_vma=False
    )
```
